32 devices in a mesh: lon: 8 (over y, x, core), lat: 4 (over z).
Axes of the slice: x: 2, y: 2, z: 4, core: 2. Of those that a mesh axis runs over, the one named last changes fastest.
Arguments:
- height_old: float32 [1024, 512], P('lon', 'lat'), may hold values from -6 to 6
- height_now: float32 [1024, 512], P('lon', 'lat'), may hold values from -6 to 6
- zonal_old: float32 [1024, 512], P('lon', 'lat'), may hold values from -6 to 6
- zonal_now: float32 [1024, 512], P('lon', 'lat'), may hold values from -6 to 6
- meridional_old: float32 [1024, 512], P('lon', 'lat'), may hold values from -6 to 6
- meridional_now: float32 [1024, 512], P('lon', 'lat'), may hold values from -6 to 6
- ocean_depth: float32 [1024, 512], P('lon', 'lat'), may hold values from 0.2 to 1
- land_sea: int32 [1024, 512], P('lon', 'lat'), may hold values 0 or 1
- metric_factor: float32 [512], P('lat'), may hold values from 0.5 to 2
- coriolis: float32 [512], P('lat'), may hold values from -0.5 to 0.5
- implicit_weight: float32 [512], replicated, may hold values from 150 to 40000
- source_longitude: int32 [512], replicated, may hold values from 0 to 1023
- source_latitude: int32 [512], replicated, may hold values from 0 to 511
- source_amplitude: float32 [512], replicated, may hold values from -24 to 24
Outputs:
- height_final: float32 [1024, 512], P('lon', 'lat')
- zonal_final: float32 [1024, 512], P('lon', 'lat')
- meridional_final: float32 [1024, 512], P('lon', 'lat')
The draws below stay inside these ranges and needn't reach their ends.
Inputs may be any that keep to these rules, and one draw needn't show every extreme that they name: `source_longitude`: cells may repeat.
All inputs are finite; a program needn't handle non-finite values. No bound on the sum of `land_sea` on one device may be relied on, other than what follows from the above.
Results may differ from the reference program's by a relative error of at most 0.0003.
Values sent between devices are 32-bit elements; how exact they have to be, the bound alone decides.
A program may use at most 64 MiB of HBM per device.

```python
import math
import jax
import jax.numpy as jnp
from jax import lax

STEPS = 1
SOURCES = 512
NLON = 1024
NLAT = 512


def draw_implicit_weight(key, part):
    phase_key, rough_key = jax.random.split(jax.random.fold_in(key, 211))
    north = jnp.arange(NLAT, dtype=jnp.float32) / NLAT
    phase = jax.random.uniform(phase_key, (), jnp.float32, 0.0, 2.0 * math.pi)
    wave = 0.5 + 0.5 * jnp.cos(4.0 * math.pi * north + phase)
    rough = jax.random.uniform(rough_key, (NLAT,), jnp.float32, 0.5, 1.0)
    level = 2.5 + 2.0 * wave
    return jnp.power(10.0, level).astype(jnp.float32) * rough


def draw_height_old(key, part):
    rough_key = jax.random.fold_in(jax.random.fold_in(key, 101), 0)
    return jax.random.truncated_normal(rough_key, -6.0, 6.0, (NLON, NLAT), jnp.float32)


def with_ends(array, own_key, least, largest):
    longest = array.shape.index(max(array.shape))
    spots = []
    for shift in (0, 1):
        where = [jax.random.randint(jax.random.fold_in(own_key, axis), (), 0, length) for axis, length in enumerate(array.shape)]
        where[longest] = (where[longest] + shift) % array.shape[longest]
        spots.append(tuple(where))
    return array.at[spots[0]].set(least).at[spots[1]].set(largest)


def levels(key, shape, cuts, least, largest):
    factor_of, own = 1.0, jax.random.fold_in(key, 6)
    for dim, blocks in cuts:
        steps = jnp.exp(jax.random.uniform(jax.random.fold_in(own, dim), (blocks,), jnp.float32, least / len(cuts), largest / len(cuts)))
        factor_of = factor_of * jnp.repeat(steps, shape[dim] // blocks).reshape([-1 if axis == dim else 1 for axis in range(len(shape))])
    return factor_of


def scatter_about(key, dims, spread, limit, cuts=(), held_as=jnp.bfloat16):
    drawn = jax.random.normal(key, dims, jnp.float32) * spread
    if len(cuts) > 0:
        drawn = levels(key, dims, cuts, -0.22, 0.18) * drawn
    return jnp.clip(drawn, min=-limit, max=limit).astype(held_as)


def setup_inputs(seed: int = 0) -> dict:
    arg_keys = jax.random.split(jax.random.key(seed), 15)
    return {
        "height_old": draw_height_old(jax.random.fold_in(arg_keys[14], 71), 0),
        "height_now": scatter_about(arg_keys[1], (NLON, NLAT), 1.0, 6.0, ((0, 8), (1, 4)), jnp.float32),
        "zonal_old": scatter_about(arg_keys[2], (NLON, NLAT), 1.0, 6.0, ((0, 8), (1, 4)), jnp.float32),
        "zonal_now": scatter_about(arg_keys[3], (NLON, NLAT), 1.0, 6.0, ((0, 8), (1, 4)), jnp.float32),
        "meridional_old": scatter_about(arg_keys[4], (NLON, NLAT), 1.0, 6.0, ((0, 8), (1, 4)), jnp.float32),
        "meridional_now": scatter_about(arg_keys[5], (NLON, NLAT), 1.0, 6.0, ((0, 8), (1, 4)), jnp.float32),
        "ocean_depth": jnp.clip(jnp.exp(math.log(1.0) - 1.609438 * jax.random.uniform(arg_keys[6], (NLON, NLAT), jnp.float32) ** levels(arg_keys[6], (NLON, NLAT), ((0, 8), (1, 4)), -0.2, 0.2)), 0.2, 1.0),
        "land_sea": with_ends((jax.random.randint(arg_keys[7], (NLON, NLAT), 0, 5) < 4).astype(jnp.int32), jax.random.fold_in(arg_keys[7], 1), 0, 1),
        "metric_factor": jnp.clip(jnp.exp(math.log(2.0) - 1.3862944 * jax.random.uniform(arg_keys[8], (NLAT,), jnp.float32) ** levels(arg_keys[8], (NLAT,), ((0, 4),), -0.2, 0.2)), 0.5, 2.0),
        "coriolis": jnp.clip(jax.random.uniform(arg_keys[9], (NLAT,), jnp.float32, -0.5, 0.5) * levels(arg_keys[9], (NLAT,), ((0, 4),), -0.4, 0.0), -0.5, 0.5),
        "implicit_weight": draw_implicit_weight(jax.random.fold_in(arg_keys[14], 71), 0),
        "source_longitude": with_ends(jax.random.randint(arg_keys[11], (SOURCES,), 0, NLON), jax.random.fold_in(arg_keys[11], 1), 0, NLON - 1).astype(jnp.int32),
        "source_latitude": with_ends(jax.random.randint(arg_keys[12], (SOURCES,), 0, NLAT), jax.random.fold_in(arg_keys[12], 1), 0, NLAT - 1).astype(jnp.int32),
        "source_amplitude": scatter_about(arg_keys[13], (SOURCES,), 4.0, 24.0, (), jnp.float32),
    }


COURANT = 0.25

def line_solve(rhs, weight):
    length = weight.shape[0]
    position = jnp.arange(length)
    lower = jnp.where(position > 0, -weight, jnp.zeros_like(weight))
    upper = jnp.where(position < length - 1, -weight, jnp.zeros_like(weight))
    middle = 1.0 + 2.0 * weight
    shape = rhs.shape
    solved = lax.linalg.tridiagonal_solve(jnp.broadcast_to(lower, shape), jnp.broadcast_to(middle, shape), jnp.broadcast_to(upper, shape), rhs[..., None])
    return solved[..., 0]

def east_diff(field):
    return jnp.roll(field, -1, 0) - jnp.roll(field, 1, 0)

def north_diff(field):
    upper = jnp.pad(field[:, 1:], ((0, 0), (0, 1)))
    lower = jnp.pad(field[:, :-1], ((0, 0), (1, 0)))
    return upper - lower

def reference(height_old, height_now, zonal_old, zonal_now, meridional_old, meridional_now, ocean_depth, land_sea, metric_factor, coriolis, implicit_weight, source_longitude, source_latitude, source_amplitude):
    wetness = land_sea.astype(height_old.dtype)
    metric = metric_factor[None, :]
    turning = coriolis[None, :]
    for _ in range(STEPS):
        flux_east = ocean_depth * wetness * zonal_now
        flux_north = ocean_depth * wetness * meridional_now
        interim = height_old - COURANT * (metric * east_diff(flux_east) + north_diff(flux_north))
        interim = interim.at[source_longitude, source_latitude].add(source_amplitude)
        zonal_next = wetness * (zonal_old - COURANT * metric * east_diff(height_now) + turning * meridional_now)
        meridional_next = wetness * (meridional_old - COURANT * north_diff(height_now) - turning * zonal_now)
        height_next = wetness * line_solve(interim, implicit_weight)
        height_old, zonal_old, meridional_old = (height_now, zonal_now, meridional_now)
        height_now, zonal_now, meridional_now = (height_next, zonal_next, meridional_next)
    return (height_now, zonal_now, meridional_now)
```

```python
import functools

import jax
import jax.numpy as jnp
from jax import lax
from jax.experimental import pallas as pl
from jax.experimental.pallas import tpu as pltpu
from jax.sharding import PartitionSpec as P

COURANT = 0.25
MESH = pl.DeviceIdType.MESH
HIGHEST = lax.Precision.HIGHEST
LAST_WITH_LAST = (((1,), (1,)), ((), ()))
FIRST_WITH_FIRST = (((0,), (0,)), ((), ()))


def exact_dot(left, right, dims):
    return lax.dot_general(left, right, dims, precision=HIGHEST, preferred_element_type=jnp.float32)


def line_factors(weight, blocks):
    padded, rows = weight.shape
    a = 1.0 / weight
    lane = lax.broadcasted_iota(jnp.int32, (padded, rows), 1)
    one = jnp.ones_like(a)
    up = (1.0 + a, a, one, one)
    down = up
    shift = 1
    while shift < rows:

        def combined(m, amount, outside):
            o = [pltpu.roll(v, amount, 1) for v in m]
            p00 = jnp.where(outside, 1.0, o[0])
            p01 = jnp.where(outside, 0.0, o[1])
            p10 = jnp.where(outside, 0.0, o[2])
            p11 = jnp.where(outside, 1.0, o[3])
            return (
                m[0] * p00 + m[1] * p10,
                m[0] * p01 + m[1] * p11,
                m[2] * p00 + m[3] * p10,
                m[2] * p01 + m[3] * p11,
            )

        up = combined(up, shift, lane < shift)
        down = combined(down, rows - shift, lane >= rows - shift)
        shift *= 2

    def carried(m, edge, order):
        m = [jnp.broadcast_to(v[:, edge : edge + 1], (padded, rows)) for v in m]
        x, y = one[:1], jnp.zeros_like(one[:1])
        xs, ys, shrink = {}, {}, {}
        for c in order:
            xs[c], ys[c] = x, y
            nx = m[0][c : c + 1] * x + m[1][c : c + 1] * y
            ny = m[2][c : c + 1] * x + m[3][c : c + 1] * y
            ratio = 1.0 / (nx + ny)
            shrink[c] = ratio
            x, y = nx * ratio, ny * ratio
        spare = [one[:1]] * (padded - blocks)
        return [jnp.concatenate([t[c] for c in range(blocks)] + spare, axis=0) for t in (xs, ys, shrink)]

    x_in, y_in, shrink_up = carried(up, rows - 1, range(blocks))
    xb_in, yb_in, shrink_down = carried(down, 0, range(blocks - 1, -1, -1))
    x = up[0] * x_in + up[1] * y_in
    y = up[2] * x_in + up[3] * y_in
    yb = down[2] * xb_in + down[3] * yb_in
    end = lambda v: jnp.broadcast_to(v[:, rows - 1 :], (padded, rows))
    start = lambda v: jnp.broadcast_to(v[:, :1], (padded, rows))
    scale = 1.0 / (end(x) + end(y) * xb_in)
    before = COURANT * pltpu.roll(end(a), 1, 0)
    after = COURANT * pltpu.roll(start(a), padded - 1, 0)
    first = lane == 0
    last = lane == rows - 1
    zero = jnp.zeros_like(a)
    return (
        a * y,
        a * yb,
        y * scale,
        yb * scale,
        shrink_up,
        shrink_down,
        jnp.where(last, after, zero) - jnp.where(first, before * y_in * shrink_up, zero),
        jnp.where(last, after * yb_in * shrink_down, zero) - jnp.where(first, before, zero),
        -jnp.where(first, before * y_in, zero),
        jnp.where(last, after * yb_in, zero),
    )


def kernel(lons, lats, *refs):
    ins, refs = refs[:14], refs[14:]
    outs, refs = refs[:3], refs[3:]
    bufs, refs = refs[:14], refs[14:]
    (
        load_sem,
        factors,
        send_lat,
        send_side,
        send_next,
        recv_lat,
        recv_side,
        recv_next,
        lat_send_sem,
        lat_recv_sem,
        side_send_sem,
        side_recv_sem,
        next_send_sem,
        next_recv_sem,
    ) = refs
    a_id = lax.axis_index("lon")
    b_id = lax.axis_index("lat")
    sides = (lax.rem(a_id + lons - 1, lons), lax.rem(a_id + 1, lons))

    barrier = pltpu.get_barrier_semaphore()
    for k in range(1, lats):
        pl.semaphore_signal(
            barrier, inc=1, device_id=(a_id, lax.rem(b_id + k, lats)), device_id_type=MESH
        )
    for k in range(lats):
        for side in sides:
            pl.semaphore_signal(
                barrier, inc=1, device_id=(side, lax.rem(b_id + k, lats)), device_id_type=MESH
            )

    loads = [None] * 14
    for k in (10, 7, 3, 5, 6, 1, 0, 8, 11, 12, 13, 2, 4, 9):
        dst = bufs[k].at[pl.ds(0, lats)] if k == 10 else bufs[k]
        loads[k] = pltpu.make_async_copy(ins[k], dst, load_sem.at[k])
        loads[k].start()
    for load in loads:
        load.wait()
    (hold, hnow, zold, znow, mold, mnow, depth, land, met, cor, wgt, slon, slat, samp) = bufs

    columns, rows = hold.shape
    padded = wgt.shape[0]
    weight = wgt[...]
    if padded > lats:
        row_id = lax.broadcasted_iota(jnp.int32, (padded, rows), 0)
        weight = jnp.where(row_id < lats, weight, 1.0)
    for k, value in enumerate(line_factors(weight, lats)):
        factors[k] = value

    def own(k, block):
        return factors[k, pl.ds(block, 1), :]

    ay, ayb, y_s, yb_s, shrink_up, shrink_down, l_f, u_f, own_l, own_u = [
        own(k, b_id) for k in range(10)
    ]

    wet = land[...].astype(jnp.float32)
    wet_depth = depth[...] * wet
    flux_east = wet_depth * znow[...]
    flux_north = wet_depth * mnow[...]
    metric = met[...]
    line = lax.broadcasted_iota(jnp.int32, (columns, rows), 0)
    lane = lax.broadcasted_iota(jnp.int32, (columns, rows), 1)

    def inner_diff(v, axis, position, size):
        ahead = jnp.where(position == size - 1, 0.0, pltpu.roll(v, size - 1, axis))
        behind = jnp.where(position == 0, 0.0, pltpu.roll(v, 1, axis))
        return ahead - behind

    rhs = hold[...] - COURANT * (
        metric * inner_diff(flux_east, 0, line, columns) + inner_diff(flux_north, 1, lane, rows)
    )
    sources = slon.shape[1]
    east_cell = lax.broadcasted_iota(jnp.int32, (columns, sources), 0) + a_id * columns
    north_cell = lax.broadcasted_iota(jnp.int32, (rows, sources), 0) + b_id * rows
    hit_east = jnp.where(east_cell == slon[...], 1.0, 0.0).astype(jnp.bfloat16)
    hit_north = north_cell == slat[...]
    rest = samp[...]
    for _ in range(3):
        piece = rest.astype(jnp.bfloat16).astype(jnp.float32)
        rest = rest - piece
        rhs = rhs + lax.dot_general(
            hit_east,
            jnp.where(hit_north, piece, 0.0).astype(jnp.bfloat16),
            LAST_WITH_LAST,
            preferred_element_type=jnp.float32,
        )

    height = hnow[...]
    row_lane = lax.broadcasted_iota(jnp.int32, (1, rows), 1)
    first_row = jnp.where(row_lane == 0, 1.0, 0.0)
    last_row = jnp.where(row_lane == rows - 1, 1.0, 0.0)
    zero_row = jnp.zeros((1, rows), jnp.float32)
    pick = jnp.concatenate(
        [
            jnp.concatenate([ay * shrink_up, zero_row, ayb * shrink_down] + [zero_row] * 5, axis=0),
            jnp.concatenate([l_f, zero_row, u_f, zero_row, own_l, own_u, zero_row, zero_row], axis=0),
            jnp.concatenate([zero_row, last_row, zero_row, first_row] + [zero_row] * 4, axis=0),
        ],
        axis=1,
    )
    moments = exact_dot(
        pick, jnp.concatenate([rhs, flux_north, height], axis=1), LAST_WITH_LAST
    )
    send_lat[0] = moments[0:2]
    send_lat[1] = moments[2:4]
    to_west = -COURANT * metric * flux_east[0:1]
    to_east = COURANT * metric * flux_east[columns - 1 :]
    line_lane = lax.broadcasted_iota(jnp.int32, (1, columns), 1)
    for side, (row, target) in enumerate(((to_west, columns - 1), (to_east, 0))):
        for way, weights in enumerate((ay * shrink_up, ayb * shrink_down)):
            total = jnp.sum(row * weights, axis=1, keepdims=True)
            send_side[side, way] = jnp.where(line_lane == target, total, 0.0)

    pl.semaphore_wait(barrier, 3 * lats - 1)
    copies = []
    for k in range(lats - 1, 0, -1):
        target = lax.rem(b_id + k, lats)
        way = jnp.where(b_id + k < lats, 0, 1)
        for side in (0, 1):
            copies.append(
                pltpu.make_async_remote_copy(
                    src_ref=send_side.at[side, way],
                    dst_ref=recv_side.at[side, lats - k - 1],
                    send_sem=side_send_sem.at[side, k - 1],
                    recv_sem=side_recv_sem.at[side, lats - k - 1],
                    device_id=(sides[side], target),
                    device_id_type=MESH,
                )
            )
            copies[-1].start()
        copies.append(
            pltpu.make_async_remote_copy(
                src_ref=send_lat.at[way],
                dst_ref=recv_lat.at[lats - k - 1],
                send_sem=lat_send_sem.at[k - 1],
                recv_sem=lat_recv_sem.at[lats - k - 1],
                device_id=(a_id, target),
                device_id_type=MESH,
            )
        )
        copies[-1].start()

    stacked = jnp.concatenate([ay, ayb] + [zero_row] * 6, axis=0)
    columns_of = jnp.transpose(stacked)
    source_lat = lax.broadcasted_iota(jnp.int32, (rows, rows), 0)
    target_lat = lax.broadcasted_iota(jnp.int32, (rows, rows), 1)
    inverse = jnp.where(
        source_lat <= target_lat, columns_of[:, 0:1] * yb_s, columns_of[:, 1:2] * y_s
    )
    plain = (((1,), (0,)), ((), ()))
    edge_solved = exact_dot(
        jnp.concatenate([to_west, to_east] + [zero_row] * 6, axis=0), inverse, plain
    )
    send_next[0] = jnp.concatenate([height[0:1], edge_solved[0:1]], axis=0)
    send_next[1] = jnp.concatenate([height[columns - 1 :], edge_solved[1:2]], axis=0)
    for side in (0, 1):
        copies.append(
            pltpu.make_async_remote_copy(
                src_ref=send_next.at[side],
                dst_ref=recv_next.at[side],
                send_sem=next_send_sem.at[side],
                recv_sem=next_recv_sem.at[side],
                device_id=(sides[side], b_id),
                device_id_type=MESH,
            )
        )
        copies[-1].start()

    solved = exact_dot(rhs, inverse, plain)
    turning = cor[...]
    zonal_part = zold[...] + turning * mnow[...] - COURANT * metric * inner_diff(height, 0, line, columns)
    meridional_part = mold[...] - COURANT * inner_diff(height, 1, lane, rows) - turning * znow[...]
    edge_line = COURANT * metric

    growth_up, growth_down = [None] * lats, [None] * lats
    product = jnp.ones((1, rows), jnp.float32)
    for d in range(lats - 1, 0, -1):
        growth_up[d] = product
        product = product * own(4, lax.rem(b_id + d, lats))
    product = jnp.ones((1, rows), jnp.float32)
    for d in range(1, lats):
        growth_down[d] = product
        product = product * own(5, lax.rem(b_id + d, lats))

    for copy in copies:
        copy.wait()

    low, high = moments[4:5], moments[5:6]
    for d in range(1, lats):
        arrived = recv_lat[d - 1, 0:1] + recv_side[0, d - 1] + recv_side[1, d - 1]
        north = b_id + d < lats
        high = high + jnp.where(north, arrived * growth_down[d][:, :1], 0.0)
        low = low + jnp.where(north, 0.0, arrived * growth_up[d][:, :1])
    south_height = jnp.where(b_id > 0, recv_lat[lats - 2, 1:2], 0.0)
    north_height = jnp.where(b_id < lats - 1, recv_lat[0, 1:2], 0.0)
    line_zero = jnp.zeros((4, columns), jnp.float32)
    corrections = exact_dot(
        jnp.concatenate([low, high, south_height, north_height, line_zero], axis=0),
        jnp.concatenate(
            [
                jnp.concatenate([yb_s, y_s] + [zero_row] * 6, axis=0),
                jnp.concatenate(
                    [zero_row, zero_row, COURANT * first_row, -COURANT * last_row] + [zero_row] * 4,
                    axis=0,
                ),
            ],
            axis=1,
        ),
        FIRST_WITH_FIRST,
    )
    from_east, from_west = recv_next[0], recv_next[1]
    at_west, at_east = line == 0, line == columns - 1
    solved = solved + corrections[:, :rows]
    solved = solved + jnp.where(at_west, from_west[1:2], 0.0) + jnp.where(at_east, from_east[1:2], 0.0)
    outs[0][...] = wet * solved
    zonal_part = (
        zonal_part
        + jnp.where(at_west, edge_line * from_west[0:1], 0.0)
        - jnp.where(at_east, edge_line * from_east[0:1], 0.0)
    )
    outs[1][...] = wet * zonal_part
    outs[2][...] = wet * (meridional_part + corrections[:, rows:])


def per_device(lons, lats, *args):
    args = list(args)
    columns, rows = args[0].shape
    sources = args[11].shape[0]
    padded = -(-lats // 8) * 8
    args[8] = args[8].reshape(1, rows)
    args[9] = args[9].reshape(1, rows)
    args[10] = args[10].reshape(lats, rows)
    for k in (11, 12, 13):
        args[k] = args[k].reshape(1, sources)
    shapes = [a.shape for a in args]
    shapes[10] = (padded, rows)
    out = jax.ShapeDtypeStruct((columns, rows), jnp.float32)
    others = lats - 1
    return pl.pallas_call(
        functools.partial(kernel, lons, lats),
        out_shape=(out, out, out),
        in_specs=[pl.BlockSpec(memory_space=pl.ANY)] * 14,
        out_specs=(pl.BlockSpec(memory_space=pltpu.VMEM),) * 3,
        scratch_shapes=[pltpu.VMEM(s, a.dtype) for s, a in zip(shapes, args)]
        + [
            pltpu.SemaphoreType.DMA((14,)),
            pltpu.VMEM((10, padded, rows), jnp.float32),
            pltpu.VMEM((2, 2, columns), jnp.float32),
            pltpu.VMEM((2, 2, 1, columns), jnp.float32),
            pltpu.VMEM((2, 2, rows), jnp.float32),
            pltpu.VMEM((others, 2, columns), jnp.float32),
            pltpu.VMEM((2, others, 1, columns), jnp.float32),
            pltpu.VMEM((2, 2, rows), jnp.float32),
            pltpu.SemaphoreType.DMA((others,)),
            pltpu.SemaphoreType.DMA((others,)),
            pltpu.SemaphoreType.DMA((2, others)),
            pltpu.SemaphoreType.DMA((2, others)),
            pltpu.SemaphoreType.DMA((2,)),
            pltpu.SemaphoreType.DMA((2,)),
        ],
        compiler_params=pltpu.CompilerParams(collective_id=0, has_side_effects=True),
    )(*args)


def solution(mesh):
    field = P("lon", "lat")
    placed = (field,) * 8 + (P("lat"),) * 2 + (P(),) * 4
    return jax.shard_map(
        functools.partial(per_device, mesh.shape["lon"], mesh.shape["lat"]),
        mesh=mesh,
        in_specs=placed,
        out_specs=(field,) * 3,
        check_vma=False,
    )
```

```python
import functools

import jax
import jax.numpy as jnp
from jax import lax
from jax.experimental import pallas as pl
from jax.experimental.pallas import tpu as pltpu
from jax.sharding import PartitionSpec as P

COURANT = 0.25
MESH = pl.DeviceIdType.MESH
HIGHEST = lax.Precision.HIGHEST
LAST_WITH_LAST = (((1,), (1,)), ((), ()))
FIRST_WITH_FIRST = (((0,), (0,)), ((), ()))


def exact_dot(left, right, dims):
    return lax.dot_general(left, right, dims, precision=HIGHEST, preferred_element_type=jnp.float32)


def line_factors(weight, blocks):
    padded, rows = weight.shape
    a = 1.0 / weight
    lane = lax.broadcasted_iota(jnp.int32, (padded, rows), 1)
    one = jnp.ones_like(a)
    up = (1.0 + a, a, one, one)
    down = up
    shift = 1
    while shift < rows:

        def combined(m, amount, outside):
            o = [pltpu.roll(v, amount, 1) for v in m]
            p00 = jnp.where(outside, 1.0, o[0])
            p01 = jnp.where(outside, 0.0, o[1])
            p10 = jnp.where(outside, 0.0, o[2])
            p11 = jnp.where(outside, 1.0, o[3])
            return (
                m[0] * p00 + m[1] * p10,
                m[0] * p01 + m[1] * p11,
                m[2] * p00 + m[3] * p10,
                m[2] * p01 + m[3] * p11,
            )

        up = combined(up, shift, lane < shift)
        down = combined(down, rows - shift, lane >= rows - shift)
        shift *= 2

    def carried(m, edge, order):
        m = [jnp.broadcast_to(v[:, edge : edge + 1], (padded, rows)) for v in m]
        x, y = one[:1], jnp.zeros_like(one[:1])
        xs, ys, shrink = {}, {}, {}
        for c in order:
            xs[c], ys[c] = x, y
            nx = m[0][c : c + 1] * x + m[1][c : c + 1] * y
            ny = m[2][c : c + 1] * x + m[3][c : c + 1] * y
            ratio = 1.0 / (nx + ny)
            shrink[c] = ratio
            x, y = nx * ratio, ny * ratio
        spare = [one[:1]] * (padded - blocks)
        return [jnp.concatenate([t[c] for c in range(blocks)] + spare, axis=0) for t in (xs, ys, shrink)]

    x_in, y_in, shrink_up = carried(up, rows - 1, range(blocks))
    xb_in, yb_in, shrink_down = carried(down, 0, range(blocks - 1, -1, -1))
    x = up[0] * x_in + up[1] * y_in
    y = up[2] * x_in + up[3] * y_in
    yb = down[2] * xb_in + down[3] * yb_in
    end = lambda v: jnp.broadcast_to(v[:, rows - 1 :], (padded, rows))
    start = lambda v: jnp.broadcast_to(v[:, :1], (padded, rows))
    scale = 1.0 / (end(x) + end(y) * xb_in)
    before = COURANT * pltpu.roll(end(a), 1, 0)
    after = COURANT * pltpu.roll(start(a), padded - 1, 0)
    first = lane == 0
    last = lane == rows - 1
    zero = jnp.zeros_like(a)
    return (
        a * y,
        a * yb,
        y * scale,
        yb * scale,
        shrink_up,
        shrink_down,
        jnp.where(last, after, zero) - jnp.where(first, before * y_in * shrink_up, zero),
        jnp.where(last, after * yb_in * shrink_down, zero) - jnp.where(first, before, zero),
        -jnp.where(first, before * y_in, zero),
        jnp.where(last, after * yb_in, zero),
    )


def kernel(lons, lats, *refs):
    ins, refs = refs[:14], refs[14:]
    outs, refs = refs[:3], refs[3:]
    bufs, refs = refs[:14], refs[14:]
    (
        load_sem,
        factors,
        send_lat,
        send_side,
        send_next,
        recv_lat,
        recv_side,
        recv_next,
        lat_send_sem,
        lat_recv_sem,
        side_send_sem,
        side_recv_sem,
        next_send_sem,
        next_recv_sem,
    ) = refs
    a_id = lax.axis_index("lon")
    b_id = lax.axis_index("lat")
    sides = (lax.rem(a_id + lons - 1, lons), lax.rem(a_id + 1, lons))

    barrier = pltpu.get_barrier_semaphore()
    for k in range(1, lats):
        pl.semaphore_signal(
            barrier, inc=1, device_id=(a_id, lax.rem(b_id + k, lats)), device_id_type=MESH
        )
    for k in range(lats):
        for side in sides:
            pl.semaphore_signal(
                barrier, inc=1, device_id=(side, lax.rem(b_id + k, lats)), device_id_type=MESH
            )

    loads = [None] * 14
    for k in (10, 7, 3, 5, 6, 1, 0, 8, 11, 12, 13, 2, 4, 9):
        dst = bufs[k].at[pl.ds(0, lats)] if k == 10 else bufs[k]
        loads[k] = pltpu.make_async_copy(ins[k], dst, load_sem.at[k])
        loads[k].start()
    for load in loads:
        load.wait()
    (hold, hnow, zold, znow, mold, mnow, depth, land, met, cor, wgt, slon, slat, samp) = bufs

    columns, rows = hold.shape
    padded = wgt.shape[0]
    weight = wgt[...]
    if padded > lats:
        row_id = lax.broadcasted_iota(jnp.int32, (padded, rows), 0)
        weight = jnp.where(row_id < lats, weight, 1.0)
    for k, value in enumerate(line_factors(weight, lats)):
        factors[k] = value

    def own(k, block):
        return factors[k, pl.ds(block, 1), :]

    ay, ayb, y_s, yb_s, shrink_up, shrink_down, l_f, u_f, own_l, own_u = [
        own(k, b_id) for k in range(10)
    ]

    wet = land[...].astype(jnp.float32)
    wet_depth = depth[...] * wet
    flux_east = wet_depth * znow[...]
    flux_north = wet_depth * mnow[...]
    metric = met[...]
    line = lax.broadcasted_iota(jnp.int32, (columns, rows), 0)
    lane = lax.broadcasted_iota(jnp.int32, (columns, rows), 1)

    def inner_diff(v, axis, position, size):
        ahead = jnp.where(position == size - 1, 0.0, pltpu.roll(v, size - 1, axis))
        behind = jnp.where(position == 0, 0.0, pltpu.roll(v, 1, axis))
        return ahead - behind

    rhs = hold[...] - COURANT * (
        metric * inner_diff(flux_east, 0, line, columns) + inner_diff(flux_north, 1, lane, rows)
    )
    sources = slon.shape[1]
    east_cell = lax.broadcasted_iota(jnp.int32, (columns, sources), 0) + a_id * columns
    north_cell = lax.broadcasted_iota(jnp.int32, (rows, sources), 0) + b_id * rows
    hit_east = jnp.where(east_cell == slon[...], 1.0, 0.0).astype(jnp.bfloat16)
    hit_north = north_cell == slat[...]
    rest = samp[...]
    for _ in range(3):
        piece = rest.astype(jnp.bfloat16).astype(jnp.float32)
        rest = rest - piece
        rhs = rhs + lax.dot_general(
            hit_east,
            jnp.where(hit_north, piece, 0.0).astype(jnp.bfloat16),
            LAST_WITH_LAST,
            preferred_element_type=jnp.float32,
        )

    height = hnow[...]
    row_lane = lax.broadcasted_iota(jnp.int32, (1, rows), 1)
    first_row = jnp.where(row_lane == 0, 1.0, 0.0)
    last_row = jnp.where(row_lane == rows - 1, 1.0, 0.0)
    zero_row = jnp.zeros((1, rows), jnp.float32)
    pick = jnp.concatenate(
        [
            jnp.concatenate([ay * shrink_up, zero_row, ayb * shrink_down] + [zero_row] * 5, axis=0),
            jnp.concatenate([l_f, zero_row, u_f, zero_row, own_l, own_u, zero_row, zero_row], axis=0),
            jnp.concatenate([zero_row, last_row, zero_row, first_row] + [zero_row] * 4, axis=0),
        ],
        axis=1,
    )
    moments = exact_dot(
        pick, jnp.concatenate([rhs, flux_north, height], axis=1), LAST_WITH_LAST
    )
    send_lat[0] = moments[0:2]
    send_lat[1] = moments[2:4]
    to_west = -COURANT * metric * flux_east[0:1]
    to_east = COURANT * metric * flux_east[columns - 1 :]
    line_lane = lax.broadcasted_iota(jnp.int32, (1, columns), 1)
    for side, (row, target) in enumerate(((to_west, columns - 1), (to_east, 0))):
        for way, weights in enumerate((ay * shrink_up, ayb * shrink_down)):
            total = jnp.sum(row * weights, axis=1, keepdims=True)
            send_side[side, way] = jnp.where(line_lane == target, total, 0.0)

    pl.semaphore_wait(barrier, 3 * lats - 1)
    copies = []
    for k in range(lats - 1, 0, -1):
        target = lax.rem(b_id + k, lats)
        way = jnp.where(b_id + k < lats, 0, 1)
        for side in (0, 1):
            copies.append(
                pltpu.make_async_remote_copy(
                    src_ref=send_side.at[side, way],
                    dst_ref=recv_side.at[side, lats - k - 1],
                    send_sem=side_send_sem.at[side, k - 1],
                    recv_sem=side_recv_sem.at[side, lats - k - 1],
                    device_id=(sides[side], target),
                    device_id_type=MESH,
                )
            )
            copies[-1].start()
        copies.append(
            pltpu.make_async_remote_copy(
                src_ref=send_lat.at[way],
                dst_ref=recv_lat.at[lats - k - 1],
                send_sem=lat_send_sem.at[k - 1],
                recv_sem=lat_recv_sem.at[lats - k - 1],
                device_id=(a_id, target),
                device_id_type=MESH,
            )
        )
        copies[-1].start()

    stacked = jnp.concatenate([ay, ayb] + [zero_row] * 6, axis=0)
    columns_of = jnp.transpose(stacked)
    source_lat = lax.broadcasted_iota(jnp.int32, (rows, rows), 0)
    target_lat = lax.broadcasted_iota(jnp.int32, (rows, rows), 1)
    inverse = jnp.where(
        source_lat <= target_lat, columns_of[:, 0:1] * yb_s, columns_of[:, 1:2] * y_s
    )
    plain = (((1,), (0,)), ((), ()))
    edge_solved = exact_dot(
        jnp.concatenate([to_west, to_east] + [zero_row] * 6, axis=0), inverse, plain
    )
    send_next[0] = jnp.concatenate([height[0:1], edge_solved[0:1]], axis=0)
    send_next[1] = jnp.concatenate([height[columns - 1 :], edge_solved[1:2]], axis=0)
    for side in (0, 1):
        copies.append(
            pltpu.make_async_remote_copy(
                src_ref=send_next.at[side],
                dst_ref=recv_next.at[side],
                send_sem=next_send_sem.at[side],
                recv_sem=next_recv_sem.at[side],
                device_id=(sides[side], b_id),
                device_id_type=MESH,
            )
        )
        copies[-1].start()

    solved = exact_dot(rhs, inverse, plain)
    turning = cor[...]
    zonal_part = zold[...] + turning * mnow[...] - COURANT * metric * inner_diff(height, 0, line, columns)
    meridional_part = mold[...] - COURANT * inner_diff(height, 1, lane, rows) - turning * znow[...]
    edge_line = COURANT * metric

    growth_up, growth_down = [None] * lats, [None] * lats
    product = jnp.ones((1, rows), jnp.float32)
    for d in range(lats - 1, 0, -1):
        growth_up[d] = product
        product = product * own(4, lax.rem(b_id + d, lats))
    product = jnp.ones((1, rows), jnp.float32)
    for d in range(1, lats):
        growth_down[d] = product
        product = product * own(5, lax.rem(b_id + d, lats))

    for copy in copies:
        copy.wait()

    low, high = moments[4:5], moments[5:6]
    for d in range(1, lats):
        arrived = recv_lat[d - 1, 0:1] + recv_side[0, d - 1] + recv_side[1, d - 1]
        north = b_id + d < lats
        high = high + jnp.where(north, arrived * growth_down[d][:, :1], 0.0)
        low = low + jnp.where(north, 0.0, arrived * growth_up[d][:, :1])
    south_height = jnp.where(b_id > 0, recv_lat[lats - 2, 1:2], 0.0)
    north_height = jnp.where(b_id < lats - 1, recv_lat[0, 1:2], 0.0)
    line_zero = jnp.zeros((4, columns), jnp.float32)
    corrections = exact_dot(
        jnp.concatenate([low, high, south_height, north_height, line_zero], axis=0),
        jnp.concatenate(
            [
                jnp.concatenate([yb_s, y_s] + [zero_row] * 6, axis=0),
                jnp.concatenate(
                    [zero_row, zero_row, COURANT * first_row, -COURANT * last_row] + [zero_row] * 4,
                    axis=0,
                ),
            ],
            axis=1,
        ),
        FIRST_WITH_FIRST,
    )
    from_east, from_west = recv_next[0], recv_next[1]
    at_west, at_east = line == 0, line == columns - 1
    solved = solved + corrections[:, :rows]
    solved = solved + jnp.where(at_west, from_west[1:2], 0.0) + jnp.where(at_east, from_east[1:2], 0.0)
    outs[0][...] = wet * solved
    zonal_part = (
        zonal_part
        + jnp.where(at_west, edge_line * from_west[0:1], 0.0)
        - jnp.where(at_east, edge_line * from_east[0:1], 0.0)
    )
    outs[1][...] = wet * zonal_part
    outs[2][...] = wet * (meridional_part + corrections[:, rows:])


def store_kernel(*refs):
    stores = [
        pltpu.make_async_copy(refs[k], refs[3 + k], refs[6].at[k]) for k in range(3)
    ]
    for store in stores:
        store.start()
    for store in stores:
        store.wait()


def per_device(lons, lats, *args):
    args = list(args)
    columns, rows = args[0].shape
    sources = args[11].shape[0]
    padded = -(-lats // 8) * 8
    args[8] = args[8].reshape(1, rows)
    args[9] = args[9].reshape(1, rows)
    args[10] = args[10].reshape(lats, rows)
    for k in (11, 12, 13):
        args[k] = args[k].reshape(1, sources)
    shapes = [a.shape for a in args]
    shapes[10] = (padded, rows)
    out = pltpu.VMEM((columns, rows), jnp.float32)
    others = lats - 1
    results = pl.pallas_call(
        functools.partial(kernel, lons, lats),
        out_shape=(out, out, out),
        in_specs=[pl.BlockSpec(memory_space=pl.ANY)] * 14,
        out_specs=(pl.BlockSpec(memory_space=pltpu.VMEM),) * 3,
        scratch_shapes=[pltpu.VMEM(s, a.dtype) for s, a in zip(shapes, args)]
        + [
            pltpu.SemaphoreType.DMA((14,)),
            pltpu.VMEM((10, padded, rows), jnp.float32),
            pltpu.VMEM((2, 2, columns), jnp.float32),
            pltpu.VMEM((2, 2, 1, columns), jnp.float32),
            pltpu.VMEM((2, 2, rows), jnp.float32),
            pltpu.VMEM((others, 2, columns), jnp.float32),
            pltpu.VMEM((2, others, 1, columns), jnp.float32),
            pltpu.VMEM((2, 2, rows), jnp.float32),
            pltpu.SemaphoreType.DMA((others,)),
            pltpu.SemaphoreType.DMA((others,)),
            pltpu.SemaphoreType.DMA((2, others)),
            pltpu.SemaphoreType.DMA((2, others)),
            pltpu.SemaphoreType.DMA((2,)),
            pltpu.SemaphoreType.DMA((2,)),
        ],
        compiler_params=pltpu.CompilerParams(collective_id=0, has_side_effects=True),
    )(*args)
    return pl.pallas_call(
        store_kernel,
        out_shape=(jax.ShapeDtypeStruct((columns, rows), jnp.float32),) * 3,
        in_specs=[pl.BlockSpec(memory_space=pltpu.VMEM)] * 3,
        out_specs=(pl.BlockSpec(memory_space=pl.ANY),) * 3,
        scratch_shapes=[pltpu.SemaphoreType.DMA((3,))],
    )(*[pltpu.with_memory_space_constraint(r, pltpu.VMEM) for r in results])


def solution(mesh):
    field = P("lon", "lat")
    placed = (field,) * 8 + (P("lat"),) * 2 + (P(),) * 4
    return jax.shard_map(
        functools.partial(per_device, mesh.shape["lon"], mesh.shape["lat"]),
        mesh=mesh,
        in_specs=placed,
        out_specs=(field,) * 3,
        check_vma=False,
    )
```

```python
import functools

import jax
import jax.numpy as jnp
from jax import lax
from jax.experimental import pallas as pl
from jax.experimental.pallas import tpu as pltpu
from jax.sharding import PartitionSpec as P

COURANT = 0.25
MESH = pl.DeviceIdType.MESH
HIGHEST = lax.Precision.HIGHEST
LAST_WITH_LAST = (((1,), (1,)), ((), ()))
FIRST_WITH_FIRST = (((0,), (0,)), ((), ()))


def exact_dot(left, right, dims):
    return lax.dot_general(left, right, dims, precision=HIGHEST, preferred_element_type=jnp.float32)


def line_factors(weight, blocks):
    padded, rows = weight.shape
    a = 1.0 / weight
    lane = lax.broadcasted_iota(jnp.int32, (padded, rows), 1)
    one = jnp.ones_like(a)
    up = (1.0 + a, a, one, one)
    down = up
    shift = 1
    while shift < rows:

        def combined(m, amount, outside):
            o = [pltpu.roll(v, amount, 1) for v in m]
            p00 = jnp.where(outside, 1.0, o[0])
            p01 = jnp.where(outside, 0.0, o[1])
            p10 = jnp.where(outside, 0.0, o[2])
            p11 = jnp.where(outside, 1.0, o[3])
            return (
                m[0] * p00 + m[1] * p10,
                m[0] * p01 + m[1] * p11,
                m[2] * p00 + m[3] * p10,
                m[2] * p01 + m[3] * p11,
            )

        up = combined(up, shift, lane < shift)
        down = combined(down, rows - shift, lane >= rows - shift)
        shift *= 2

    def carried(m, edge, order):
        m = [jnp.broadcast_to(v[:, edge : edge + 1], (padded, rows)) for v in m]
        x, y = one[:1], jnp.zeros_like(one[:1])
        xs, ys, shrink = {}, {}, {}
        for c in order:
            xs[c], ys[c] = x, y
            nx = m[0][c : c + 1] * x + m[1][c : c + 1] * y
            ny = m[2][c : c + 1] * x + m[3][c : c + 1] * y
            ratio = 1.0 / (nx + ny)
            shrink[c] = ratio
            x, y = nx * ratio, ny * ratio
        spare = [one[:1]] * (padded - blocks)
        return [jnp.concatenate([t[c] for c in range(blocks)] + spare, axis=0) for t in (xs, ys, shrink)]

    x_in, y_in, shrink_up = carried(up, rows - 1, range(blocks))
    xb_in, yb_in, shrink_down = carried(down, 0, range(blocks - 1, -1, -1))
    x = up[0] * x_in + up[1] * y_in
    y = up[2] * x_in + up[3] * y_in
    yb = down[2] * xb_in + down[3] * yb_in
    end = lambda v: jnp.broadcast_to(v[:, rows - 1 :], (padded, rows))
    start = lambda v: jnp.broadcast_to(v[:, :1], (padded, rows))
    scale = 1.0 / (end(x) + end(y) * xb_in)
    before = COURANT * pltpu.roll(end(a), 1, 0)
    after = COURANT * pltpu.roll(start(a), padded - 1, 0)
    first = lane == 0
    last = lane == rows - 1
    zero = jnp.zeros_like(a)
    return (
        a * y,
        a * yb,
        y * scale,
        yb * scale,
        shrink_up,
        shrink_down,
        jnp.where(last, after, zero) - jnp.where(first, before * y_in * shrink_up, zero),
        jnp.where(last, after * yb_in * shrink_down, zero) - jnp.where(first, before, zero),
        -jnp.where(first, before * y_in, zero),
        jnp.where(last, after * yb_in, zero),
    )


def kernel(lons, lats, *refs):
    ins, refs = refs[:14], refs[14:]
    outs, refs = refs[:3], refs[3:]
    bufs, refs = refs[:14], refs[14:]
    (
        load_sem,
        factors,
        send_lat,
        send_side,
        send_next,
        recv_lat,
        recv_side,
        recv_next,
        lat_send_sem,
        lat_recv_sem,
        side_send_sem,
        side_recv_sem,
        next_send_sem,
        next_recv_sem,
    ) = refs
    a_id = lax.axis_index("lon")
    b_id = lax.axis_index("lat")
    sides = (lax.rem(a_id + lons - 1, lons), lax.rem(a_id + 1, lons))

    barrier = pltpu.get_barrier_semaphore()
    loads = [
        pltpu.make_async_copy(
            ins[k], bufs[k].at[pl.ds(0, lats)] if k == 10 else bufs[k], load_sem.at[k]
        )
        for k in range(14)
    ]
    early, late = (3, 6, 7, 8, 1, 10), (5, 0, 11, 12, 13, 2, 4, 9)
    for side in sides:
        pl.semaphore_signal(barrier, inc=1, device_id=(side, b_id), device_id_type=MESH)
    for k in early + late:
        loads[k].start()
    for k in range(1, lats):
        other = lax.rem(b_id + k, lats)
        for column in (*sides, a_id):
            pl.semaphore_signal(barrier, inc=1, device_id=(column, other), device_id_type=MESH)
    (hold, hnow, zold, znow, mold, mnow, depth, land, met, cor, wgt, slon, slat, samp) = bufs
    columns, rows = hold.shape
    padded = wgt.shape[0]
    for k in early:
        loads[k].wait()

    scaled_metric = COURANT * met[...]
    for side, (at, sign) in enumerate(((0, -1.0), (columns - 1, 1.0))):
        edge = pl.ds(at, 1)
        flux = depth[edge, :] * land[edge, :].astype(jnp.float32) * znow[edge, :]
        flux = sign * scaled_metric * flux
        send_side[side] = flux
        send_next[side] = jnp.concatenate([flux, hnow[edge, :]], axis=0)

    weight = wgt[...]
    if padded > lats:
        row_id = lax.broadcasted_iota(jnp.int32, (padded, rows), 0)
        weight = jnp.where(row_id < lats, weight, 1.0)
    for k, value in enumerate(line_factors(weight, lats)):
        factors[k] = value

    pl.semaphore_wait(barrier, 3 * lats - 1)
    side_copies, copies = [], []
    for k in range(lats - 1, 0, -1):
        for side in (0, 1):
            side_copies.append(
                pltpu.make_async_remote_copy(
                    src_ref=send_side.at[side],
                    dst_ref=recv_side.at[side, lats - k - 1],
                    send_sem=side_send_sem.at[side, k - 1],
                    recv_sem=side_recv_sem.at[side, lats - k - 1],
                    device_id=(sides[side], lax.rem(b_id + k, lats)),
                    device_id_type=MESH,
                )
            )
            side_copies[-1].start()
    for side in (0, 1):
        copies.append(
            pltpu.make_async_remote_copy(
                src_ref=send_next.at[side],
                dst_ref=recv_next.at[side],
                send_sem=next_send_sem.at[side],
                recv_sem=next_recv_sem.at[side],
                device_id=(sides[side], b_id),
                device_id_type=MESH,
            )
        )
        copies[-1].start()
    for k in late:
        loads[k].wait()

    def own(k, block):
        return factors[k, pl.ds(block, 1), :]

    ay, ayb, y_s, yb_s, shrink_up, shrink_down, l_f, u_f, own_l, own_u = [
        own(k, b_id) for k in range(10)
    ]

    wet = land[...].astype(jnp.float32)
    wet_depth = depth[...] * wet
    flux_east = wet_depth * znow[...]
    flux_north = wet_depth * mnow[...]
    metric = met[...]
    line = lax.broadcasted_iota(jnp.int32, (columns, rows), 0)
    lane = lax.broadcasted_iota(jnp.int32, (columns, rows), 1)

    def inner_diff(v, axis, position, size):
        ahead = jnp.where(position == size - 1, 0.0, pltpu.roll(v, size - 1, axis))
        behind = jnp.where(position == 0, 0.0, pltpu.roll(v, 1, axis))
        return ahead - behind

    rhs = hold[...] - COURANT * (
        metric * inner_diff(flux_east, 0, line, columns) + inner_diff(flux_north, 1, lane, rows)
    )
    sources = slon.shape[1]
    east_cell = lax.broadcasted_iota(jnp.int32, (columns, sources), 0) + a_id * columns
    north_cell = lax.broadcasted_iota(jnp.int32, (rows, sources), 0) + b_id * rows
    hit_east = jnp.where(east_cell == slon[...], 1.0, 0.0).astype(jnp.bfloat16)
    hit_north = north_cell == slat[...]
    rest = samp[...]
    for _ in range(3):
        piece = rest.astype(jnp.bfloat16).astype(jnp.float32)
        rest = rest - piece
        rhs = rhs + lax.dot_general(
            hit_east,
            jnp.where(hit_north, piece, 0.0).astype(jnp.bfloat16),
            LAST_WITH_LAST,
            preferred_element_type=jnp.float32,
        )

    height = hnow[...]
    row_lane = lax.broadcasted_iota(jnp.int32, (1, rows), 1)
    first_row = jnp.where(row_lane == 0, 1.0, 0.0)
    last_row = jnp.where(row_lane == rows - 1, 1.0, 0.0)
    zero_row = jnp.zeros((1, rows), jnp.float32)
    pick = jnp.concatenate(
        [
            jnp.concatenate([ay * shrink_up, zero_row, ayb * shrink_down] + [zero_row] * 5, axis=0),
            jnp.concatenate([l_f, zero_row, u_f, zero_row, own_l, own_u, zero_row, zero_row], axis=0),
            jnp.concatenate([zero_row, last_row, zero_row, first_row] + [zero_row] * 4, axis=0),
        ],
        axis=1,
    )
    moments = exact_dot(
        pick, jnp.concatenate([rhs, flux_north, height], axis=1), LAST_WITH_LAST
    )
    send_lat[0] = moments[0:2]
    send_lat[1] = moments[2:4]
    for k in range(lats - 1, 0, -1):
        copies.append(
            pltpu.make_async_remote_copy(
                src_ref=send_lat.at[jnp.where(b_id + k < lats, 0, 1)],
                dst_ref=recv_lat.at[lats - k - 1],
                send_sem=lat_send_sem.at[k - 1],
                recv_sem=lat_recv_sem.at[lats - k - 1],
                device_id=(a_id, lax.rem(b_id + k, lats)),
                device_id_type=MESH,
            )
        )
        copies[-1].start()

    stacked = jnp.concatenate([ay, ayb] + [zero_row] * 6, axis=0)
    columns_of = jnp.transpose(stacked)
    source_lat = lax.broadcasted_iota(jnp.int32, (rows, rows), 0)
    target_lat = lax.broadcasted_iota(jnp.int32, (rows, rows), 1)
    inverse = jnp.where(
        source_lat <= target_lat, columns_of[:, 0:1] * yb_s, columns_of[:, 1:2] * y_s
    )
    plain = (((1,), (0,)), ((), ()))
    solved = exact_dot(rhs, inverse, plain)
    turning = cor[...]
    zonal_part = zold[...] + turning * mnow[...] - COURANT * metric * inner_diff(height, 0, line, columns)
    meridional_part = mold[...] - COURANT * inner_diff(height, 1, lane, rows) - turning * znow[...]

    growth, reach = [None] * lats, [None] * lats
    up_product = jnp.ones((1, rows), jnp.float32)
    for d in range(lats - 1, 0, -1):
        block = lax.rem(b_id + d, lats)
        growth[d] = up_product
        up_product = up_product * own(4, block)
        reach[d] = own(0, block) * up_product
    down_product = jnp.ones((1, rows), jnp.float32)
    for d in range(1, lats):
        block = lax.rem(b_id + d, lats)
        north = b_id + d < lats
        growth[d] = jnp.where(north, down_product, growth[d])
        down_product = down_product * own(5, block)
        reach[d] = jnp.where(north, own(1, block) * down_product, reach[d])

    for copy in copies:
        copy.wait()

    low, high = moments[4:5], moments[5:6]
    for d in range(1, lats):
        arrived = recv_lat[d - 1, 0:1] * growth[d][:, :1]
        north = b_id + d < lats
        high = high + jnp.where(north, arrived, 0.0)
        low = low + jnp.where(north, 0.0, arrived)
    south_height = jnp.where(b_id > 0, recv_lat[lats - 2, 1:2], 0.0)
    north_height = jnp.where(b_id < lats - 1, recv_lat[0, 1:2], 0.0)
    line_zero = jnp.zeros((4, columns), jnp.float32)
    corrections = exact_dot(
        jnp.concatenate([low, high, south_height, north_height, line_zero], axis=0),
        jnp.concatenate(
            [
                jnp.concatenate([yb_s, y_s] + [zero_row] * 6, axis=0),
                jnp.concatenate(
                    [zero_row, zero_row, COURANT * first_row, -COURANT * last_row] + [zero_row] * 4,
                    axis=0,
                ),
            ],
            axis=1,
        ),
        FIRST_WITH_FIRST,
    )
    from_east, from_west = recv_next[0], recv_next[1]
    edge_solved = exact_dot(
        jnp.concatenate([from_west[0:1], from_east[0:1]] + [zero_row] * 6, axis=0), inverse, plain
    )
    at_west, at_east = line == 0, line == columns - 1
    solved = solved + corrections[:, :rows]
    outs[0][...] = wet * solved
    zonal_part = (
        zonal_part
        + jnp.where(at_west, scaled_metric * from_west[1:2], 0.0)
        - jnp.where(at_east, scaled_metric * from_east[1:2], 0.0)
    )
    outs[1][...] = wet * zonal_part
    outs[2][...] = wet * (meridional_part + corrections[:, rows:])

    for copy in side_copies:
        copy.wait()
    terms = []
    for side in (1, 0):
        low, high = zero_row, zero_row
        for d in range(1, lats):
            arrived = recv_side[side, d - 1] * reach[d]
            north = b_id + d < lats
            high = high + jnp.where(north, arrived, 0.0)
            low = low + jnp.where(north, 0.0, arrived)
        terms += [low, high]
    sums = jnp.sum(jnp.concatenate(terms + [zero_row] * 4, axis=0), axis=1, keepdims=True)
    for k, at in enumerate((0, columns - 1)):
        edge = pl.ds(at, 1)
        outs[0][edge, :] = wet[at : at + 1] * (
            solved[at : at + 1]
            + edge_solved[k : k + 1]
            + sums[2 * k : 2 * k + 1] * yb_s
            + sums[2 * k + 1 : 2 * k + 2] * y_s
        )


def store_kernel(*refs):
    stores = [
        pltpu.make_async_copy(refs[k], refs[3 + k], refs[6].at[k]) for k in range(3)
    ]
    for store in stores:
        store.start()
    for store in stores:
        store.wait()


def per_device(lons, lats, *args):
    args = list(args)
    columns, rows = args[0].shape
    sources = args[11].shape[0]
    padded = -(-lats // 8) * 8
    args[8] = args[8].reshape(1, rows)
    args[9] = args[9].reshape(1, rows)
    args[10] = args[10].reshape(lats, rows)
    for k in (11, 12, 13):
        args[k] = args[k].reshape(1, sources)
    shapes = [a.shape for a in args]
    shapes[10] = (padded, rows)
    out = pltpu.VMEM((columns, rows), jnp.float32)
    others = lats - 1
    results = pl.pallas_call(
        functools.partial(kernel, lons, lats),
        out_shape=(out, out, out),
        in_specs=[pl.BlockSpec(memory_space=pl.ANY)] * 14,
        out_specs=(pl.BlockSpec(memory_space=pltpu.VMEM),) * 3,
        scratch_shapes=[pltpu.VMEM(s, a.dtype) for s, a in zip(shapes, args)]
        + [
            pltpu.SemaphoreType.DMA((14,)),
            pltpu.VMEM((10, padded, rows), jnp.float32),
            pltpu.VMEM((2, 2, columns), jnp.float32),
            pltpu.VMEM((2, 1, rows), jnp.float32),
            pltpu.VMEM((2, 2, rows), jnp.float32),
            pltpu.VMEM((others, 2, columns), jnp.float32),
            pltpu.VMEM((2, others, 1, rows), jnp.float32),
            pltpu.VMEM((2, 2, rows), jnp.float32),
            pltpu.SemaphoreType.DMA((others,)),
            pltpu.SemaphoreType.DMA((others,)),
            pltpu.SemaphoreType.DMA((2, others)),
            pltpu.SemaphoreType.DMA((2, others)),
            pltpu.SemaphoreType.DMA((2,)),
            pltpu.SemaphoreType.DMA((2,)),
        ],
        compiler_params=pltpu.CompilerParams(collective_id=0, has_side_effects=True),
    )(*args)
    return pl.pallas_call(
        store_kernel,
        out_shape=(jax.ShapeDtypeStruct((columns, rows), jnp.float32),) * 3,
        in_specs=[pl.BlockSpec(memory_space=pltpu.VMEM)] * 3,
        out_specs=(pl.BlockSpec(memory_space=pl.ANY),) * 3,
        scratch_shapes=[pltpu.SemaphoreType.DMA((3,))],
    )(*[pltpu.with_memory_space_constraint(r, pltpu.VMEM) for r in results])


def solution(mesh):
    field = P("lon", "lat")
    placed = (field,) * 8 + (P("lat"),) * 2 + (P(),) * 4
    return jax.shard_map(
        functools.partial(per_device, mesh.shape["lon"], mesh.shape["lat"]),
        mesh=mesh,
        in_specs=placed,
        out_specs=(field,) * 3,
        check_vma=False,
    )
```

```python
import functools

import jax
import jax.numpy as jnp
from jax import lax
from jax.experimental import pallas as pl
from jax.experimental.pallas import tpu as pltpu
from jax.sharding import PartitionSpec as P

COURANT = 0.25
MESH = pl.DeviceIdType.MESH
HIGHEST = lax.Precision.HIGHEST
LAST_WITH_LAST = (((1,), (1,)), ((), ()))
FIRST_WITH_FIRST = (((0,), (0,)), ((), ()))


def exact_dot(left, right, dims):
    return lax.dot_general(left, right, dims, precision=HIGHEST, preferred_element_type=jnp.float32)


def line_factors(weight, blocks):
    padded, rows = weight.shape
    a = 1.0 / weight
    lane = lax.broadcasted_iota(jnp.int32, (padded, rows), 1)
    one = jnp.ones_like(a)
    up = (1.0 + a, a, one, one)
    down = up
    shift = 1
    while shift < rows:

        def combined(m, amount, outside):
            o = [pltpu.roll(v, amount, 1) for v in m]
            p00 = jnp.where(outside, 1.0, o[0])
            p01 = jnp.where(outside, 0.0, o[1])
            p10 = jnp.where(outside, 0.0, o[2])
            p11 = jnp.where(outside, 1.0, o[3])
            return (
                m[0] * p00 + m[1] * p10,
                m[0] * p01 + m[1] * p11,
                m[2] * p00 + m[3] * p10,
                m[2] * p01 + m[3] * p11,
            )

        up = combined(up, shift, lane < shift)
        down = combined(down, rows - shift, lane >= rows - shift)
        shift *= 2

    def carried(m, edge, order):
        m = [jnp.broadcast_to(v[:, edge : edge + 1], (padded, rows)) for v in m]
        x, y = one[:1], jnp.zeros_like(one[:1])
        xs, ys, shrink = {}, {}, {}
        for c in order:
            xs[c], ys[c] = x, y
            nx = m[0][c : c + 1] * x + m[1][c : c + 1] * y
            ny = m[2][c : c + 1] * x + m[3][c : c + 1] * y
            ratio = 1.0 / (nx + ny)
            shrink[c] = ratio
            x, y = nx * ratio, ny * ratio
        spare = [one[:1]] * (padded - blocks)
        return [jnp.concatenate([t[c] for c in range(blocks)] + spare, axis=0) for t in (xs, ys, shrink)]

    x_in, y_in, shrink_up = carried(up, rows - 1, range(blocks))
    xb_in, yb_in, shrink_down = carried(down, 0, range(blocks - 1, -1, -1))
    x = up[0] * x_in + up[1] * y_in
    y = up[2] * x_in + up[3] * y_in
    yb = down[2] * xb_in + down[3] * yb_in
    end = lambda v: jnp.broadcast_to(v[:, rows - 1 :], (padded, rows))
    start = lambda v: jnp.broadcast_to(v[:, :1], (padded, rows))
    scale = 1.0 / (end(x) + end(y) * xb_in)
    before = COURANT * pltpu.roll(end(a), 1, 0)
    after = COURANT * pltpu.roll(start(a), padded - 1, 0)
    first = lane == 0
    last = lane == rows - 1
    zero = jnp.zeros_like(a)
    return (
        a * y,
        a * yb,
        y * scale,
        yb * scale,
        shrink_up,
        shrink_down,
        jnp.where(last, after, zero) - jnp.where(first, before * y_in * shrink_up, zero),
        jnp.where(last, after * yb_in * shrink_down, zero) - jnp.where(first, before, zero),
        -jnp.where(first, before * y_in, zero),
        jnp.where(last, after * yb_in, zero),
    )


def kernel(lons, lats, *refs):
    ins, refs = refs[:14], refs[14:]
    outs, refs = refs[:3], refs[3:]
    bufs, refs = refs[:14], refs[14:]
    (
        load_sem,
        factors,
        send_lat,
        send_side,
        send_next,
        recv_lat,
        recv_side,
        recv_next,
        lat_send_sem,
        lat_recv_sem,
        side_send_sem,
        side_recv_sem,
        next_send_sem,
        next_recv_sem,
    ) = refs
    a_id = lax.axis_index("lon")
    b_id = lax.axis_index("lat")
    sides = (lax.rem(a_id + lons - 1, lons), lax.rem(a_id + 1, lons))

    barrier = pltpu.get_barrier_semaphore()
    loads = [
        pltpu.make_async_copy(
            ins[k], bufs[k].at[pl.ds(0, lats)] if k == 10 else bufs[k], load_sem.at[k]
        )
        for k in range(14)
    ]
    early, late = (3, 6, 7, 8, 1), (5, 0, 11, 12, 13, 2, 4, 9)
    for side in sides:
        pl.semaphore_signal(barrier, inc=1, device_id=(side, b_id), device_id_type=MESH)
    for k in (*early, 10, *late):
        loads[k].start()
    for k in range(1, lats):
        other = lax.rem(b_id + k, lats)
        for column in (*sides, a_id):
            pl.semaphore_signal(barrier, inc=1, device_id=(column, other), device_id_type=MESH)
    (hold, hnow, zold, znow, mold, mnow, depth, land, met, cor, wgt, slon, slat, samp) = bufs
    columns, rows = hold.shape
    padded = wgt.shape[0]
    for k in early:
        loads[k].wait()

    scaled_metric = COURANT * met[...]
    for side, (at, sign) in enumerate(((0, -1.0), (columns - 1, 1.0))):
        edge = pl.ds(at, 1)
        flux = depth[edge, :] * land[edge, :].astype(jnp.float32) * znow[edge, :]
        flux = sign * scaled_metric * flux
        send_side[side] = flux
        send_next[side] = jnp.concatenate([flux, hnow[edge, :]], axis=0)

    pl.semaphore_wait(barrier, 3 * lats - 1)
    side_copies, copies = [], []
    for k in range(lats - 1, 0, -1):
        for side in (0, 1):
            side_copies.append(
                pltpu.make_async_remote_copy(
                    src_ref=send_side.at[side],
                    dst_ref=recv_side.at[side, lats - k - 1],
                    send_sem=side_send_sem.at[side, k - 1],
                    recv_sem=side_recv_sem.at[side, lats - k - 1],
                    device_id=(sides[side], lax.rem(b_id + k, lats)),
                    device_id_type=MESH,
                )
            )
            side_copies[-1].start()
    for side in (0, 1):
        copies.append(
            pltpu.make_async_remote_copy(
                src_ref=send_next.at[side],
                dst_ref=recv_next.at[side],
                send_sem=next_send_sem.at[side],
                recv_sem=next_recv_sem.at[side],
                device_id=(sides[side], b_id),
                device_id_type=MESH,
            )
        )
        copies[-1].start()
    loads[10].wait()
    weight = wgt[...]
    if padded > lats:
        row_id = lax.broadcasted_iota(jnp.int32, (padded, rows), 0)
        weight = jnp.where(row_id < lats, weight, 1.0)
    for k, value in enumerate(line_factors(weight, lats)):
        factors[k] = value

    for k in late:
        loads[k].wait()

    def own(k, block):
        return factors[k, pl.ds(block, 1), :]

    ay, ayb, y_s, yb_s, shrink_up, shrink_down, l_f, u_f, own_l, own_u = [
        own(k, b_id) for k in range(10)
    ]

    wet = land[...].astype(jnp.float32)
    wet_depth = depth[...] * wet
    flux_east = wet_depth * znow[...]
    flux_north = wet_depth * mnow[...]
    metric = met[...]
    line = lax.broadcasted_iota(jnp.int32, (columns, rows), 0)
    lane = lax.broadcasted_iota(jnp.int32, (columns, rows), 1)

    def inner_diff(v, axis, position, size):
        ahead = jnp.where(position == size - 1, 0.0, pltpu.roll(v, size - 1, axis))
        behind = jnp.where(position == 0, 0.0, pltpu.roll(v, 1, axis))
        return ahead - behind

    rhs = hold[...] - COURANT * (
        metric * inner_diff(flux_east, 0, line, columns) + inner_diff(flux_north, 1, lane, rows)
    )
    sources = slon.shape[1]
    east_cell = lax.broadcasted_iota(jnp.int32, (columns, sources), 0) + a_id * columns
    north_cell = lax.broadcasted_iota(jnp.int32, (rows, sources), 0) + b_id * rows
    hit_east = jnp.where(east_cell == slon[...], 1.0, 0.0).astype(jnp.bfloat16)
    hit_north = north_cell == slat[...]
    rest = samp[...]
    for _ in range(3):
        piece = rest.astype(jnp.bfloat16).astype(jnp.float32)
        rest = rest - piece
        rhs = rhs + lax.dot_general(
            hit_east,
            jnp.where(hit_north, piece, 0.0).astype(jnp.bfloat16),
            LAST_WITH_LAST,
            preferred_element_type=jnp.float32,
        )

    height = hnow[...]
    row_lane = lax.broadcasted_iota(jnp.int32, (1, rows), 1)
    first_row = jnp.where(row_lane == 0, 1.0, 0.0)
    last_row = jnp.where(row_lane == rows - 1, 1.0, 0.0)
    zero_row = jnp.zeros((1, rows), jnp.float32)
    pick = jnp.concatenate(
        [
            jnp.concatenate([ay * shrink_up, zero_row, ayb * shrink_down] + [zero_row] * 5, axis=0),
            jnp.concatenate([l_f, zero_row, u_f, zero_row, own_l, own_u, zero_row, zero_row], axis=0),
            jnp.concatenate([zero_row, last_row, zero_row, first_row] + [zero_row] * 4, axis=0),
        ],
        axis=1,
    )
    moments = exact_dot(
        pick, jnp.concatenate([rhs, flux_north, height], axis=1), LAST_WITH_LAST
    )
    send_lat[0] = moments[0:2]
    send_lat[1] = moments[2:4]
    for k in range(lats - 1, 0, -1):
        copies.append(
            pltpu.make_async_remote_copy(
                src_ref=send_lat.at[jnp.where(b_id + k < lats, 0, 1)],
                dst_ref=recv_lat.at[lats - k - 1],
                send_sem=lat_send_sem.at[k - 1],
                recv_sem=lat_recv_sem.at[lats - k - 1],
                device_id=(a_id, lax.rem(b_id + k, lats)),
                device_id_type=MESH,
            )
        )
        copies[-1].start()

    stacked = jnp.concatenate([ay, ayb] + [zero_row] * 6, axis=0)
    columns_of = jnp.transpose(stacked)
    source_lat = lax.broadcasted_iota(jnp.int32, (rows, rows), 0)
    target_lat = lax.broadcasted_iota(jnp.int32, (rows, rows), 1)
    inverse = jnp.where(
        source_lat <= target_lat, columns_of[:, 0:1] * yb_s, columns_of[:, 1:2] * y_s
    )
    plain = (((1,), (0,)), ((), ()))
    solved = exact_dot(rhs, inverse, plain)
    turning = cor[...]
    zonal_part = zold[...] + turning * mnow[...] - COURANT * metric * inner_diff(height, 0, line, columns)
    meridional_part = mold[...] - COURANT * inner_diff(height, 1, lane, rows) - turning * znow[...]

    growth, reach = [None] * lats, [None] * lats
    up_product = jnp.ones((1, rows), jnp.float32)
    for d in range(lats - 1, 0, -1):
        block = lax.rem(b_id + d, lats)
        growth[d] = up_product
        up_product = up_product * own(4, block)
        reach[d] = own(0, block) * up_product
    down_product = jnp.ones((1, rows), jnp.float32)
    for d in range(1, lats):
        block = lax.rem(b_id + d, lats)
        north = b_id + d < lats
        growth[d] = jnp.where(north, down_product, growth[d])
        down_product = down_product * own(5, block)
        reach[d] = jnp.where(north, own(1, block) * down_product, reach[d])

    for copy in copies:
        copy.wait()

    low, high = moments[4:5], moments[5:6]
    for d in range(1, lats):
        arrived = recv_lat[d - 1, 0:1] * growth[d][:, :1]
        north = b_id + d < lats
        high = high + jnp.where(north, arrived, 0.0)
        low = low + jnp.where(north, 0.0, arrived)
    south_height = jnp.where(b_id > 0, recv_lat[lats - 2, 1:2], 0.0)
    north_height = jnp.where(b_id < lats - 1, recv_lat[0, 1:2], 0.0)
    line_zero = jnp.zeros((4, columns), jnp.float32)
    corrections = exact_dot(
        jnp.concatenate([low, high, south_height, north_height, line_zero], axis=0),
        jnp.concatenate(
            [
                jnp.concatenate([yb_s, y_s] + [zero_row] * 6, axis=0),
                jnp.concatenate(
                    [zero_row, zero_row, COURANT * first_row, -COURANT * last_row] + [zero_row] * 4,
                    axis=0,
                ),
            ],
            axis=1,
        ),
        FIRST_WITH_FIRST,
    )
    from_east, from_west = recv_next[0], recv_next[1]
    edge_solved = exact_dot(
        jnp.concatenate([from_west[0:1], from_east[0:1]] + [zero_row] * 6, axis=0), inverse, plain
    )
    at_west, at_east = line == 0, line == columns - 1
    solved = solved + corrections[:, :rows]
    outs[0][...] = wet * solved
    zonal_part = (
        zonal_part
        + jnp.where(at_west, scaled_metric * from_west[1:2], 0.0)
        - jnp.where(at_east, scaled_metric * from_east[1:2], 0.0)
    )
    outs[1][...] = wet * zonal_part
    outs[2][...] = wet * (meridional_part + corrections[:, rows:])

    for copy in side_copies:
        copy.wait()
    terms = []
    for side in (1, 0):
        low, high = zero_row, zero_row
        for d in range(1, lats):
            arrived = recv_side[side, d - 1] * reach[d]
            north = b_id + d < lats
            high = high + jnp.where(north, arrived, 0.0)
            low = low + jnp.where(north, 0.0, arrived)
        terms += [low, high]
    sums = jnp.sum(jnp.concatenate(terms + [zero_row] * 4, axis=0), axis=1, keepdims=True)
    for k, at in enumerate((0, columns - 1)):
        edge = pl.ds(at, 1)
        outs[0][edge, :] = wet[at : at + 1] * (
            solved[at : at + 1]
            + edge_solved[k : k + 1]
            + sums[2 * k : 2 * k + 1] * yb_s
            + sums[2 * k + 1 : 2 * k + 2] * y_s
        )


def store_kernel(*refs):
    stores = [
        pltpu.make_async_copy(refs[k], refs[3 + k], refs[6].at[k]) for k in range(3)
    ]
    for store in stores:
        store.start()
    for store in stores:
        store.wait()


def per_device(lons, lats, *args):
    args = list(args)
    columns, rows = args[0].shape
    sources = args[11].shape[0]
    padded = -(-lats // 8) * 8
    args[8] = args[8].reshape(1, rows)
    args[9] = args[9].reshape(1, rows)
    args[10] = args[10].reshape(lats, rows)
    for k in (11, 12, 13):
        args[k] = args[k].reshape(1, sources)
    shapes = [a.shape for a in args]
    shapes[10] = (padded, rows)
    out = pltpu.VMEM((columns, rows), jnp.float32)
    others = lats - 1
    results = pl.pallas_call(
        functools.partial(kernel, lons, lats),
        out_shape=(out, out, out),
        in_specs=[pl.BlockSpec(memory_space=pl.ANY)] * 14,
        out_specs=(pl.BlockSpec(memory_space=pltpu.VMEM),) * 3,
        scratch_shapes=[pltpu.VMEM(s, a.dtype) for s, a in zip(shapes, args)]
        + [
            pltpu.SemaphoreType.DMA((14,)),
            pltpu.VMEM((10, padded, rows), jnp.float32),
            pltpu.VMEM((2, 2, columns), jnp.float32),
            pltpu.VMEM((2, 1, rows), jnp.float32),
            pltpu.VMEM((2, 2, rows), jnp.float32),
            pltpu.VMEM((others, 2, columns), jnp.float32),
            pltpu.VMEM((2, others, 1, rows), jnp.float32),
            pltpu.VMEM((2, 2, rows), jnp.float32),
            pltpu.SemaphoreType.DMA((others,)),
            pltpu.SemaphoreType.DMA((others,)),
            pltpu.SemaphoreType.DMA((2, others)),
            pltpu.SemaphoreType.DMA((2, others)),
            pltpu.SemaphoreType.DMA((2,)),
            pltpu.SemaphoreType.DMA((2,)),
        ],
        compiler_params=pltpu.CompilerParams(collective_id=0, has_side_effects=True),
    )(*args)
    return pl.pallas_call(
        store_kernel,
        out_shape=(jax.ShapeDtypeStruct((columns, rows), jnp.float32),) * 3,
        in_specs=[pl.BlockSpec(memory_space=pltpu.VMEM)] * 3,
        out_specs=(pl.BlockSpec(memory_space=pl.ANY),) * 3,
        scratch_shapes=[pltpu.SemaphoreType.DMA((3,))],
    )(*[pltpu.with_memory_space_constraint(r, pltpu.VMEM) for r in results])


def solution(mesh):
    field = P("lon", "lat")
    placed = (field,) * 8 + (P("lat"),) * 2 + (P(),) * 4
    return jax.shard_map(
        functools.partial(per_device, mesh.shape["lon"], mesh.shape["lat"]),
        mesh=mesh,
        in_specs=placed,
        out_specs=(field,) * 3,
        check_vma=False,
    )
```
